32 devices in a mesh: dp: 4 (over y, core), seq: 8 (over z, x).
Axes of the slice: x: 2, y: 2, z: 4, core: 2. Of those that a mesh axis runs over, the one named last changes fastest.
Arguments:
- queries: bfloat16 [4, 4096, 1024], P('dp', 'seq'), may hold values from -6 to 6
- key_vectors: bfloat16 [4, 4096, 1024], P('dp', 'seq'), may hold values from -6 to 6
- value_vectors: bfloat16 [4, 4096, 2048], P('dp', 'seq'), may hold values from -6 to 6
- grad_output: bfloat16 [4, 4096, 2048], P('dp', 'seq'), may hold values from -0.375 to 0.375
- log_gate: float32 [4, 4096, 1024], P('dp', 'seq'), may hold values from -1 to 0, as said below
- layer_input: bfloat16 [4, 4096, 2048], P('dp', 'seq'), may hold values from -0.0625 to 0.0625
Outputs:
- grad_queries: bfloat16 [4, 4096, 1024], P('dp', 'seq')
- grad_keys: bfloat16 [4, 4096, 1024], P('dp', 'seq')
- grad_values: bfloat16 [4, 4096, 2048], P('dp', 'seq')
- grad_log_gate: float32 [4, 4096, 1024], P('dp', 'seq')
- grad_key_weight: float32 [2048, 1024], P(('dp', 'seq'))
The draws below stay inside these ranges and needn't reach their ends.
Inputs may be any that keep to these rules, and one draw needn't show every extreme that they name: `log_gate`: every entry is negative.
All inputs are finite; a program needn't handle non-finite values.
Results may differ from the reference program's by a relative error of at most 0.03.
Values sent between devices are 32-bit elements; how exact they have to be, the bound alone decides.
A program may use at most 192 MiB of HBM per device.

```python
import jax
import jax.numpy as jnp
from jax import lax

D = 2048
HEADS = 4
DK = 256
DV = 512
GROUP = 64
TOK_DEV = 512
BATCH_SEQUENCES = 4
SEQUENCE_LENGTH = 4096


def draw_log_gate(key, part):
    width = HEADS * DK
    blocks = SEQUENCE_LENGTH // TOK_DEV
    portion_random_key, gradual_random_key, quick_random_key, device_random_key, coarse_random_key, spike_random_key, objective_random_key, regime_random_key = jax.random.split(key, 8)
    share = 0.5
    rough = jnp.exp(jax.random.uniform(coarse_random_key, (BATCH_SEQUENCES, blocks, TOK_DEV, width), jnp.float32, jnp.log(0.6), jnp.log(1.6)))
    slow_mask = jax.random.bernoulli(portion_random_key, share, (BATCH_SEQUENCES, 1, 1, width))
    fast_here = jax.random.bernoulli(regime_random_key, 0.5, (BATCH_SEQUENCES, blocks, 1, width))
    stays_slow = jnp.logical_or(slow_mask, jnp.logical_not(fast_here))
    slow_rate = jnp.exp(jax.random.uniform(gradual_random_key, (BATCH_SEQUENCES, 1, 1, width), jnp.float32, jnp.log(0.02), jnp.log(0.2))) * jnp.log(10.0) / SEQUENCE_LENGTH
    fast_rate = jnp.exp(jax.random.uniform(quick_random_key, (BATCH_SEQUENCES, 1, 1, width), jnp.float32, jnp.log(1.0 / 50.0), jnp.log(1.0 / 30.0)))
    base_rate = jnp.where(stays_slow, slow_rate, fast_rate)
    device_factor = jnp.exp(jax.random.uniform(device_random_key, (BATCH_SEQUENCES, blocks, 1, width), jnp.float32, jnp.log(0.7), jnp.log(1.4)))
    rate_full = (base_rate * device_factor * rough).reshape(BATCH_SEQUENCES, SEQUENCE_LENGTH, width)
    spike_position = jax.random.randint(spike_random_key, (BATCH_SEQUENCES, 3), 0, SEQUENCE_LENGTH)
    position_index = lax.broadcasted_iota(jnp.int32, (BATCH_SEQUENCES, SEQUENCE_LENGTH), 1)
    affected_rows = jnp.any(position_index[:, :, None] == spike_position[:, None, :], axis=2)
    losses = jax.random.uniform(objective_random_key, (BATCH_SEQUENCES, SEQUENCE_LENGTH, width), jnp.float32, jnp.log(0.4), jnp.log(0.8))
    return (jnp.where(affected_rows[:, :, None], losses, 0.0) - rate_full).astype(jnp.float32)


def spiked(values, key, source, target, blocks, factor):
    def block_of(dim):
        return (jnp.arange(values.shape[dim]) // (values.shape[dim] // blocks)).reshape((-1,) + (1,) * (values.ndim - 1 - dim))

    first = jax.random.permutation(key, blocks)[block_of(target)]
    second = (block_of(target) + blocks // 2) % blocks
    return jnp.where((block_of(source) == first) | (block_of(source) == second), factor * values, values)


def shard_levels(rng, dims, cuts, least, largest):
    factor_of, own = 1.0, jax.random.fold_in(rng, 6)
    for position, blocks in cuts:
        steps = jnp.exp(jax.random.uniform(jax.random.fold_in(own, position), (blocks,), jnp.float32, least / len(cuts), largest / len(cuts)))
        factor_of = factor_of * jnp.repeat(steps, dims[position] // blocks).reshape([-1 if axis == position else 1 for axis in range(len(dims))])
    return factor_of


def bell_draw(stream_key, dims, spread, most, cuts=(), held_as=jnp.bfloat16):
    values = jax.random.normal(stream_key, dims, jnp.float32) * spread
    if len(cuts) > 0:
        values = shard_levels(stream_key, dims, cuts, -0.22, 0.18) * values
    return jnp.clip(values, min=-most, max=most).astype(held_as)


def heavy_noise(own_key, extent, spread, limit, pieces, heavy, held_as=jnp.bfloat16):
    drawn = spread * jax.random.normal(own_key, extent, jnp.float32)
    if pieces:
        drawn = drawn * shard_levels(own_key, extent, pieces, -0.22, 0.18)
    return jnp.clip(spiked(drawn, jax.random.fold_in(own_key, 3), *heavy), -limit, limit).astype(held_as)


def setup_inputs(seed: int = 0) -> dict:
    arg_keys = jax.random.split(jax.random.key(seed), 7)
    queries = bell_draw(arg_keys[0], (BATCH_SEQUENCES, SEQUENCE_LENGTH, HEADS * DK), 1.0, 6.0, ((0, 4), (1, 8)))
    key_vectors = bell_draw(arg_keys[1], (BATCH_SEQUENCES, SEQUENCE_LENGTH, HEADS * DK), 1.0, 6.0, ((0, 4), (1, 8)))
    value_vectors = bell_draw(arg_keys[2], (BATCH_SEQUENCES, SEQUENCE_LENGTH, HEADS * DV), 1.0, 6.0, ((0, 4), (1, 8)))
    grad_output = bell_draw(arg_keys[3], (BATCH_SEQUENCES, SEQUENCE_LENGTH, HEADS * DV), (SEQUENCE_LENGTH // 16) ** -0.5, 0.375, ((0, 4), (1, 8)))
    log_gate = draw_log_gate(jax.random.fold_in(arg_keys[6], 71), 0)
    layer_input = heavy_noise(arg_keys[5], (BATCH_SEQUENCES, SEQUENCE_LENGTH, D), (BATCH_SEQUENCES * SEQUENCE_LENGTH) ** -0.5, 0.0625, ((0, 4), (1, 8)), (1, 2, 8, 2.0))
    return {"queries": queries, "key_vectors": key_vectors, "value_vectors": value_vectors, "grad_output": grad_output, "log_gate": log_gate, "layer_input": layer_input}


def widened(first_op, second_op):
    low_pair = lax.optimization_barrier((first_op.astype(jnp.bfloat16), second_op.astype(jnp.bfloat16)))
    return low_pair[0].astype(jnp.float32), low_pair[1].astype(jnp.float32)


def product(pattern, first_op, second_op):
    first_wide, second_wide = widened(first_op, second_op)
    return jnp.einsum(pattern, first_wide, second_wide, precision=lax.Precision.HIGHEST)


def reference(queries, key_vectors, value_vectors, grad_output, log_gate, layer_input):
    blocks = SEQUENCE_LENGTH // GROUP
    key_scale = DK ** -0.5

    def as_blocks(array, width):
        shaped = array.astype(jnp.float32).reshape(BATCH_SEQUENCES, blocks, GROUP, HEADS, width)
        return jnp.transpose(shaped, (1, 0, 2, 3, 4))

    def as_rows(array, width):
        return jnp.transpose(array, (1, 0, 2, 3, 4)).reshape(BATCH_SEQUENCES, SEQUENCE_LENGTH, HEADS * width)

    query_rows = as_blocks(queries, DK)
    key_rows = as_blocks(key_vectors, DK)
    value_rows = as_blocks(value_vectors, DV)
    cotan_rows = as_blocks(grad_output, DV)
    block_cums = jnp.cumsum(as_blocks(log_gate, DK), axis=2)
    lower_mask = (lax.broadcasted_iota(jnp.int32, (GROUP, GROUP), 0) >= lax.broadcasted_iota(jnp.int32, (GROUP, GROUP), 1)).astype(jnp.float32)

    def forward_block(carry_state, block):
        key_part, value_part, cotan_part, cum_part = block
        cum_end = cum_part[:, -1]
        pair_dot = product("bthj,bshj->bhts", cotan_part, value_part) * lower_mask
        grad_q = key_scale * jnp.exp(cum_part) * (product("bthj,bhij->bthi", cotan_part, carry_state) + product("bhts,bshi->bthi", pair_dot, key_part * jnp.exp(-cum_part)))
        carry_state = carry_state * jnp.exp(cum_end)[..., None] + product("bshi,bshj->bhij", key_part * jnp.exp(cum_end[:, None] - cum_part), value_part)
        return carry_state, grad_q

    def backward_block(back_state, block):
        query_part, key_part, value_part, cotan_part, cum_part = block
        cum_end = cum_part[:, -1]
        query_up = query_part * jnp.exp(cum_part)
        key_down = key_part * jnp.exp(-cum_part)
        key_end = key_part * jnp.exp(cum_end[:, None] - cum_part)
        scores = key_scale * product("bthi,bshi->bhts", query_up, key_down) * lower_mask
        pair_dot = product("bthj,bshj->bhts", cotan_part, value_part) * lower_mask
        grad_k = key_scale * jnp.exp(-cum_part) * product("bhts,bthi->bshi", pair_dot, query_up) + jnp.exp(cum_end[:, None] - cum_part) * product("bshj,bhij->bshi", value_part, back_state)
        grad_v = product("bhts,bthj->bshj", scores, cotan_part) + product("bshi,bhij->bshj", key_end, back_state)
        back_state = back_state * jnp.exp(cum_end)[..., None] + key_scale * product("bthi,bthj->bhij", query_up, cotan_part)
        return back_state, (grad_k, grad_v)

    zero_state = jnp.zeros((BATCH_SEQUENCES, HEADS, DK, DV), jnp.float32)
    grad_q = lax.scan(forward_block, zero_state, (key_rows, value_rows, cotan_rows, block_cums))[1]
    grad_k, grad_v = lax.scan(backward_block, zero_state, (query_rows, key_rows, value_rows, cotan_rows, block_cums), reverse=True)[1]
    log_drift = query_rows * grad_q - key_rows * grad_k
    grad_log_gate = lax.cumsum(as_rows(log_drift, DK), axis=1, reverse=True)
    grad_keys = as_rows(grad_k, DK).astype(jnp.bfloat16)
    input_wide = layer_input.reshape(BATCH_SEQUENCES * SEQUENCE_LENGTH, D).astype(jnp.float32)
    keys_wide = grad_keys.reshape(BATCH_SEQUENCES * SEQUENCE_LENGTH, HEADS * DK).astype(jnp.float32)
    grad_key_weight = jnp.dot(jnp.transpose(input_wide), keys_wide, precision=lax.Precision.HIGHEST)
    return (as_rows(grad_q, DK).astype(jnp.bfloat16), grad_keys, as_rows(grad_v, DV).astype(jnp.bfloat16), grad_log_gate, grad_key_weight)
```

```python
import functools

import jax
import jax.numpy as jnp
from jax import lax
from jax.experimental import pallas as pl
from jax.experimental.pallas import tpu as pltpu
from jax.sharding import PartitionSpec as P

HEADS = 4
DK = 256
DV = 512
ROWS = 64
NT = (((1,), (1,)), ((), ()))
TN = (((0,), (0,)), ((), ()))
NN = (((1,), (0,)), ((), ()))


def mm(first_op, second_op, dims):
    return lax.dot_general(
        first_op.astype(jnp.bfloat16),
        second_op.astype(jnp.bfloat16),
        dims,
        preferred_element_type=jnp.float32,
    )


def block_of(length):
    return 128 if length % 128 == 0 else 64


def triangle(size, lower):
    row = lax.broadcasted_iota(jnp.int32, (size, size), 0)
    col = lax.broadcasted_iota(jnp.int32, (size, size), 1)
    return (row >= col) if lower else (row <= col)


def exact_sum(ones, values):
    high = values.astype(jnp.bfloat16)
    rest = values - high.astype(jnp.float32)
    middle = rest.astype(jnp.bfloat16)
    low = (rest - middle.astype(jnp.float32)).astype(jnp.bfloat16)
    return mm(ones, high, NN) + (mm(ones, middle, NN) + mm(ones, low, NN))


def states_kernel(q_ref, k_ref, v_ref, g_ref, lg_ref, decay_ref, f_ref, b_ref):
    length = q_ref.shape[0]
    size = block_of(length)
    ones = triangle(size, True).astype(jnp.bfloat16)
    base = jnp.zeros((1, DK), jnp.float32)
    cums = []
    for n in range(length // size):
        part = exact_sum(ones, lg_ref[n * size : (n + 1) * size, :]) + base
        base = part[size - 1 :, :]
        cums.append(part)
    cum = jnp.concatenate(cums, axis=0)
    decay_ref[...] = jnp.broadcast_to(jnp.exp(base), decay_ref.shape)
    key_end = k_ref[...].astype(jnp.float32) * jnp.exp(base - cum)
    query_up = q_ref[...].astype(jnp.float32) * jnp.exp(cum)
    f_ref[...] = mm(v_ref[...], key_end, TN)
    b_ref[...] = DK**-0.5 * mm(g_ref[...], query_up, TN)


def chain_kernel(
    count, decay_ref, f_ref, b_ref, fin_ref, bin_ref, f_out, b_out, f_send, f_recv, b_send, b_recv
):
    place = lax.axis_index("seq")
    right = lax.rem(place + 1, count)
    left = lax.rem(place + count - 1, count)
    chunks = f_ref.shape[0] // ROWS
    per_head = chunks // HEADS
    barrier = pltpu.get_barrier_semaphore()
    for peer in (left, right):
        pl.semaphore_signal(
            barrier, inc=1, device_id={"seq": peer}, device_id_type=pl.DeviceIdType.MESH
        )
    pl.semaphore_wait(barrier, 2)

    def copy(c, out, into, send, recv, peer):
        rows = pl.ds(pl.multiple_of(c * ROWS, ROWS), ROWS)
        return pltpu.make_async_remote_copy(
            src_ref=out.at[rows],
            dst_ref=into.at[rows],
            send_sem=send.at[c],
            recv_sem=recv.at[c],
            device_id={"seq": peer},
            device_id_type=pl.DeviceIdType.MESH,
        )

    def advance(c, own, out, into, send, recv, peer, is_first, is_last):
        rows = pl.ds(pl.multiple_of(c * ROWS, ROWS), ROWS)

        @pl.when(is_first)
        def _():
            into[rows, :] = jnp.zeros((ROWS, DK), jnp.float32)

        @pl.when(jnp.logical_not(is_first))
        def _():
            copy(c, out, into, send, recv, peer).wait_recv()

        @pl.when(jnp.logical_not(is_last))
        def _():
            decay = decay_ref[pl.ds((c // per_head) * 8, 8), :][0:1, :]
            out[rows, :] = decay * into[rows, :] + own[rows, :]
            copy(c, out, into, send, recv, peer).start()

    at_low, at_high = place == 0, place == count - 1

    def step(t, _):
        ahead = t - place
        back = t - (count - 1 - place)

        @pl.when((ahead >= 0) & (ahead < chunks))
        def _():
            advance(ahead, f_ref, f_out, fin_ref, f_send, f_recv, right, at_low, at_high)

        @pl.when((back >= 0) & (back < chunks))
        def _():
            advance(back, b_ref, b_out, bin_ref, b_send, b_recv, left, at_high, at_low)

        return 0

    lax.fori_loop(0, chunks + count - 1, step, 0)

    def drain(c, _):
        @pl.when(jnp.logical_not(at_high))
        def _():
            copy(c, f_out, fin_ref, f_send, f_recv, right).wait_send()

        @pl.when(jnp.logical_not(at_low))
        def _():
            copy(c, b_out, bin_ref, b_send, b_recv, left).wait_send()

        return 0

    lax.fori_loop(0, chunks, drain, 0)


def grads_kernel(
    q_ref, k_ref, v_ref, g_ref, lg_ref, fin_ref, bin_ref, dq_ref, dk_ref, dv_ref, gate_ref, dq_full
):
    length = q_ref.shape[0]
    size = block_of(length)
    scale = DK**-0.5
    lower = triangle(size, True)
    sum_down = lower.astype(jnp.bfloat16)
    sum_up = triangle(size, False).astype(jnp.bfloat16)
    state = fin_ref[...]
    back = bin_ref[...]
    kept = []
    for n in range(length // size):
        at = slice(n * size, (n + 1) * size)
        cum = exact_sum(sum_down, lg_ref[at, :])
        end = cum[size - 1 :, :]
        middle = cum[size // 2 - 1 : size // 2, :]
        rise = jnp.exp(cum - middle)
        fall = jnp.exp(middle - cum)
        key = k_ref[at, :].astype(jnp.float32)
        pair = jnp.where(lower, mm(g_ref[at, :], v_ref[at, :], NT), 0.0).astype(jnp.bfloat16)
        dq = scale * (
            jnp.exp(cum) * mm(g_ref[at, :], state, NN) + rise * mm(pair, key * fall, NN)
        )
        dq_full[at, :] = dq
        dq_ref[at, :] = dq.astype(jnp.bfloat16)
        state = state * jnp.exp(end) + mm(v_ref[at, :], key * jnp.exp(end - cum), TN)
        kept.append((cum, pair))
    tail = jnp.sum(state * back, axis=0, keepdims=True)
    for n in reversed(range(length // size)):
        at = slice(n * size, (n + 1) * size)
        cum, pair = kept[n]
        end = cum[size - 1 :, :]
        middle = cum[size // 2 - 1 : size // 2, :]
        rise = jnp.exp(cum - middle)
        fall = jnp.exp(middle - cum)
        to_end = jnp.exp(end - cum)
        query = q_ref[at, :].astype(jnp.float32)
        key = k_ref[at, :].astype(jnp.float32)
        query_rise = (query * rise).astype(jnp.bfloat16)
        scores = jnp.where(lower, scale * mm(query_rise, key * fall, NT), 0.0)
        dk = scale * fall * mm(pair, query_rise, TN) + to_end * mm(v_ref[at, :], back, NN)
        dv = mm(scores, g_ref[at, :], TN) + mm(key * to_end, back, NT)
        dk_ref[at, :] = dk.astype(jnp.bfloat16)
        dv_ref[at, :] = dv.astype(jnp.bfloat16)
        sums = exact_sum(sum_up, query * dq_full[at, :] - key * dk) + tail
        gate_ref[at, :] = sums
        tail = sums[0:1, :]
        back = back * jnp.exp(end) + scale * mm(
            g_ref[at, :], query * jnp.exp(cum), TN
        )


def shards(count, queries, key_vectors, value_vectors, grad_output, log_gate, layer_input):
    length = queries.shape[1]
    f32, bf16 = jnp.float32, jnp.bfloat16
    thin = pl.BlockSpec((length, DK), lambda h: (0, h))
    wide = pl.BlockSpec((length, DV), lambda h: (0, h))
    carry = pl.BlockSpec((DV, DK), lambda h: (h, 0))
    rows = (queries[0], key_vectors[0], value_vectors[0], grad_output[0], log_gate[0])
    work = length * DK * DV * HEADS
    decay, forward, backward = pl.pallas_call(
        states_kernel,
        grid=(HEADS,),
        in_specs=[thin, thin, wide, wide, thin],
        out_specs=[pl.BlockSpec((8, DK), lambda h: (h, 0)), carry, carry],
        out_shape=[
            jax.ShapeDtypeStruct((HEADS * 8, DK), f32),
            jax.ShapeDtypeStruct((HEADS * DV, DK), f32),
            jax.ShapeDtypeStruct((HEADS * DV, DK), f32),
        ],
        cost_estimate=pl.CostEstimate(
            flops=4 * work, bytes_accessed=length * HEADS * 24 * DK, transcendentals=0
        ),
        name="states",
    )(*rows)
    chunks = HEADS * DV // ROWS
    vmem = pl.BlockSpec(memory_space=pltpu.VMEM)
    incoming, outgoing = pl.pallas_call(
        functools.partial(chain_kernel, count),
        in_specs=[vmem] * 3,
        out_specs=[vmem] * 2,
        out_shape=[jax.ShapeDtypeStruct((HEADS * DV, DK), f32)] * 2,
        scratch_shapes=[pltpu.VMEM((HEADS * DV, DK), f32)] * 2
        + [pltpu.SemaphoreType.DMA((chunks,))] * 4,
        compiler_params=pltpu.CompilerParams(collective_id=0, has_side_effects=True),
        name="chain",
    )(decay, forward, backward)
    grad_q, grad_k, grad_v, grad_gate = pl.pallas_call(
        grads_kernel,
        grid=(HEADS,),
        in_specs=[thin, thin, wide, wide, thin, carry, carry],
        out_specs=[thin, thin, wide, thin],
        out_shape=[
            jax.ShapeDtypeStruct((length, HEADS * DK), bf16),
            jax.ShapeDtypeStruct((length, HEADS * DK), bf16),
            jax.ShapeDtypeStruct((length, HEADS * DV), bf16),
            jax.ShapeDtypeStruct((length, HEADS * DK), f32),
        ],
        scratch_shapes=[pltpu.VMEM((length, DK), f32)],
        cost_estimate=pl.CostEstimate(
            flops=16 * work, bytes_accessed=length * HEADS * 40 * DK, transcendentals=0
        ),
        name="grads",
    )(*rows, incoming, outgoing)
    grad_key_weight = lax.psum_scatter(
        lax.dot_general(layer_input[0], grad_k, TN, preferred_element_type=f32),
        ("dp", "seq"),
        scatter_dimension=0,
        tiled=True,
    )
    return (grad_q[None], grad_k[None], grad_v[None], grad_gate[None], grad_key_weight)


def solution(mesh):
    rows = P("dp", "seq", None)
    return jax.shard_map(
        functools.partial(shards, mesh.shape["seq"]),
        mesh=mesh,
        in_specs=(rows,) * 6,
        out_specs=(rows, rows, rows, rows, P(("dp", "seq"), None)),
        check_vma=False,
    )
```

```python
import functools

import jax
import jax.numpy as jnp
from jax import lax
from jax.experimental import pallas as pl
from jax.experimental.pallas import tpu as pltpu
from jax.sharding import PartitionSpec as P

HEADS = 4
DK = 256
DV = 512
ROWS = 64
LANES = 128
NT = (((1,), (1,)), ((), ()))
TN = (((0,), (0,)), ((), ()))
NN = (((1,), (0,)), ((), ()))


def mm(first_op, second_op, dims):
    return lax.dot_general(
        first_op.astype(jnp.bfloat16),
        second_op.astype(jnp.bfloat16),
        dims,
        preferred_element_type=jnp.float32,
    )


def block_of(length):
    return 128 if length % 128 == 0 else 64


def triangle(size, lower):
    row = lax.broadcasted_iota(jnp.int32, (size, size), 0)
    col = lax.broadcasted_iota(jnp.int32, (size, size), 1)
    return (row >= col) if lower else (row <= col)


def exact_sum(ones, values):
    high = values.astype(jnp.bfloat16)
    rest = values - high.astype(jnp.float32)
    middle = rest.astype(jnp.bfloat16)
    low = (rest - middle.astype(jnp.float32)).astype(jnp.bfloat16)
    return mm(ones, high, NN) + (mm(ones, middle, NN) + mm(ones, low, NN))


def states_kernel(q_ref, k_ref, v_ref, g_ref, lg_ref, decay_ref, f_ref, b_ref):
    length = q_ref.shape[0]
    size = block_of(length)
    ones = triangle(size, True).astype(jnp.bfloat16)
    base = jnp.zeros((1, DK), jnp.float32)
    cums = []
    for n in range(length // size):
        part = exact_sum(ones, lg_ref[n * size : (n + 1) * size, :]) + base
        base = part[size - 1 :, :]
        cums.append(part)
    cum = jnp.concatenate(cums, axis=0)
    decay_ref[...] = jnp.broadcast_to(jnp.exp(base), decay_ref.shape)
    key_end = k_ref[...].astype(jnp.float32) * jnp.exp(base - cum)
    query_up = q_ref[...].astype(jnp.float32) * jnp.exp(cum)
    f_ref[...] = mm(v_ref[...], key_end, TN)
    b_ref[...] = DK**-0.5 * mm(g_ref[...], query_up, TN)


def chain_kernel(
    count, decay_ref, f_ref, b_ref, fin_ref, bin_ref, f_out, b_out, f_send, f_recv, b_send, b_recv
):
    place = lax.axis_index("seq")
    right = lax.rem(place + 1, count)
    left = lax.rem(place + count - 1, count)
    chunks = f_ref.shape[0] // ROWS
    per_head = chunks // HEADS
    barrier = pltpu.get_barrier_semaphore()
    for peer in (left, right):
        pl.semaphore_signal(
            barrier, inc=1, device_id={"seq": peer}, device_id_type=pl.DeviceIdType.MESH
        )
    pl.semaphore_wait(barrier, 2)

    def copy(c, out, into, send, recv, peer):
        rows = pl.ds(pl.multiple_of(c * ROWS, ROWS), ROWS)
        return pltpu.make_async_remote_copy(
            src_ref=out.at[rows],
            dst_ref=into.at[rows],
            send_sem=send.at[c],
            recv_sem=recv.at[c],
            device_id={"seq": peer},
            device_id_type=pl.DeviceIdType.MESH,
        )

    def advance(c, own, out, into, send, recv, peer, is_first, is_last):
        rows = pl.ds(pl.multiple_of(c * ROWS, ROWS), ROWS)

        @pl.when(is_first)
        def _():
            into[rows, :] = jnp.zeros((ROWS, DK), jnp.float32)

        @pl.when(jnp.logical_not(is_first))
        def _():
            copy(c, out, into, send, recv, peer).wait_recv()

        @pl.when(jnp.logical_not(is_last))
        def _():
            decay = decay_ref[pl.ds((c // per_head) * 8, 8), :][0:1, :]
            out[rows, :] = decay * into[rows, :] + own[rows, :]
            copy(c, out, into, send, recv, peer).start()

    at_low, at_high = place == 0, place == count - 1

    def step(t, _):
        ahead = t - place
        back = t - (count - 1 - place)

        @pl.when((ahead >= 0) & (ahead < chunks))
        def _():
            advance(ahead, f_ref, f_out, fin_ref, f_send, f_recv, right, at_low, at_high)

        @pl.when((back >= 0) & (back < chunks))
        def _():
            advance(back, b_ref, b_out, bin_ref, b_send, b_recv, left, at_high, at_low)

        return 0

    lax.fori_loop(0, chunks + count - 1, step, 0)

    def drain(c, _):
        @pl.when(jnp.logical_not(at_high))
        def _():
            copy(c, f_out, fin_ref, f_send, f_recv, right).wait_send()

        @pl.when(jnp.logical_not(at_low))
        def _():
            copy(c, b_out, bin_ref, b_send, b_recv, left).wait_send()

        return 0

    lax.fori_loop(0, chunks, drain, 0)


def grads_kernel(
    q_ref, k_ref, v_ref, g_ref, lg_ref, fin_ref, bin_ref, dq_ref, dk_ref, dv_ref, gate_ref, dq_full
):
    length = q_ref.shape[0]
    size = block_of(length)
    scale = DK**-0.5
    lower = triangle(size, True)
    sum_down = lower.astype(jnp.bfloat16)
    sum_up = triangle(size, False).astype(jnp.bfloat16)
    state = fin_ref[...]
    back = bin_ref[...]
    kept = []
    for n in range(length // size):
        at = slice(n * size, (n + 1) * size)
        cum = exact_sum(sum_down, lg_ref[at, :])
        end = cum[size - 1 :, :]
        middle = cum[size // 2 - 1 : size // 2, :]
        rise = jnp.exp(cum - middle)
        fall = jnp.exp(middle - cum)
        key = k_ref[at, :].astype(jnp.float32)
        pair = jnp.where(lower, mm(g_ref[at, :], v_ref[at, :], NT), 0.0).astype(jnp.bfloat16)
        dq = scale * (
            jnp.exp(cum) * mm(g_ref[at, :], state, NN) + rise * mm(pair, key * fall, NN)
        )
        dq_full[at, :] = dq
        dq_ref[at, :] = dq.astype(jnp.bfloat16)
        state = state * jnp.exp(end) + mm(v_ref[at, :], key * jnp.exp(end - cum), TN)
        kept.append((cum, pair))
    tail = jnp.sum(state * back, axis=0, keepdims=True)
    for n in reversed(range(length // size)):
        at = slice(n * size, (n + 1) * size)
        cum, pair = kept[n]
        end = cum[size - 1 :, :]
        middle = cum[size // 2 - 1 : size // 2, :]
        rise = jnp.exp(cum - middle)
        fall = jnp.exp(middle - cum)
        to_end = jnp.exp(end - cum)
        query = q_ref[at, :].astype(jnp.float32)
        key = k_ref[at, :].astype(jnp.float32)
        query_rise = (query * rise).astype(jnp.bfloat16)
        scores = jnp.where(lower, scale * mm(query_rise, key * fall, NT), 0.0)
        dk = scale * fall * mm(pair, query_rise, TN) + to_end * mm(v_ref[at, :], back, NN)
        dv = mm(scores, g_ref[at, :], TN) + mm(key * to_end, back, NT)
        dk_ref[at, :] = dk.astype(jnp.bfloat16)
        dv_ref[at, :] = dv.astype(jnp.bfloat16)
        sums = exact_sum(sum_up, query * dq_full[at, :] - key * dk) + tail
        gate_ref[at, :] = sums
        tail = sums[0:1, :]
        back = back * jnp.exp(end) + scale * mm(
            g_ref[at, :], query * jnp.exp(cum), TN
        )


def weight_kernel(x_ref, k_ref, out_ref):
    total = mm(x_ref[...], k_ref[...], TN)
    for c in range(out_ref.shape[0]):
        out_ref[c] = total[:, c * LANES : (c + 1) * LANES]


def scatter_kernel(sizes, part_ref, out_ref, *scratch):
    wide, high, low = sizes
    r0, s0, ry1, sy1, ry2, rb1, sb1, rb2, s2, r3, send, recv = scratch
    chunks = part_ref.shape[0]
    dp, seq = lax.axis_index("dp"), lax.axis_index("seq")
    y, core = dp // 2, dp % 2
    a, b = seq // low, seq % low
    other = 1 - core

    def peers(axis):
        me, size = {"y": (y, wide), "b": (b, low), "a": (a, high)}[axis]
        return [lax.rem(me + k, size) for k in range(1, size)]

    def device(axis, value):
        place = {"y": y, "core": core, "a": a, "b": b} | {axis: value}
        return {"dp": place["y"] * 2 + place["core"], "seq": place["a"] * low + place["b"]}

    barrier = pltpu.get_barrier_semaphore()
    reached = [device("core", other)]
    for axis in ("y", "b", "a"):
        reached += [device(axis, p) for p in peers(axis)]
    for target in reached:
        pl.semaphore_signal(
            barrier, inc=1, device_id=target, device_id_type=pl.DeviceIdType.MESH
        )
    pl.semaphore_wait(barrier, len(reached))

    def copies(c, stage, axis, source, into):
        made = []
        for k, peer in enumerate([other] if axis == "core" else peers(axis)):
            made.append(
                pltpu.make_async_remote_copy(
                    src_ref=source(peer),
                    dst_ref=into(k),
                    send_sem=send.at[stage, c, k],
                    recv_sem=recv.at[stage, c, k],
                    device_id=device(axis, peer),
                    device_id_type=pl.DeviceIdType.MESH,
                )
            )
        return made

    def stage_of(c, stage):
        half = c // 2
        y_first = c % 2 == 0
        if stage == 0:
            return copies(c, 0, "core", lambda p: part_ref.at[c, :, p], lambda k: r0.at[c])
        if stage == 1 and y_first:
            return copies(c, 1, "y", lambda p: s0.at[c, p], lambda k: ry1.at[half, k])
        if stage == 1:
            return copies(c, 1, "b", lambda p: s0.at[c, :, :, p], lambda k: rb1.at[half, k])
        if stage == 2 and y_first:
            return copies(c, 2, "b", lambda p: sy1.at[half, :, p], lambda k: ry2.at[half, k])
        if stage == 2:
            return copies(c, 2, "y", lambda p: sb1.at[half, p], lambda k: rb2.at[half, k])
        return copies(c, 3, "a", lambda p: s2.at[c, p], lambda k: r3.at[c, k])

    def landed(c, stage):
        half = c // 2
        y_first = c % 2 == 0
        for one in stage_of(c, stage):
            one.wait_recv()
        if stage == 0:
            s0[c] = part_ref[c, :, core] + r0[c]
        elif stage == 1 and y_first:
            sy1[half] = sum((ry1[half, k] for k in range(wide - 1)), s0[c, y])
        elif stage == 1:
            sb1[half] = sum((rb1[half, k] for k in range(low - 1)), s0[c, :, :, b])
        elif stage == 2 and y_first:
            s2[c] = sum((ry2[half, k] for k in range(low - 1)), sy1[half, :, b])
        elif stage == 2:
            s2[c] = sum((rb2[half, k] for k in range(wide - 1)), sb1[half, y])
        else:
            out_ref[:, c * LANES : (c + 1) * LANES] = sum(
                (r3[c, k] for k in range(high - 1)), s2[c, a]
            )

    def begin(c, stage):
        for one in stage_of(c, stage):
            one.start()

    for c in range(chunks):
        begin(c, 0)
    for c in range(chunks):
        landed(c, 0)
        begin(c, 1)
    for t in range(chunks + 2):
        for stage in (1, 2, 3):
            c = t - stage + 1
            if 0 <= c < chunks:
                landed(c, stage)
                if stage < 3:
                    begin(c, stage + 1)
    for c in range(chunks):
        for stage in range(4):
            for one in stage_of(c, stage):
                one.wait_send()


def weight_sum(counts, layer_rows, grad_k):
    length, model = layer_rows.shape
    columns = grad_k.shape[1]
    ranks, count = counts
    chunks = columns // LANES
    tall = min(256, model)
    part = pl.pallas_call(
        weight_kernel,
        grid=(model // tall,),
        in_specs=[
            pl.BlockSpec((length, tall), lambda i: (0, i)),
            pl.BlockSpec((length, columns), lambda i: (0, 0)),
        ],
        out_specs=pl.BlockSpec((chunks, tall, LANES), lambda i: (0, i, 0)),
        out_shape=jax.ShapeDtypeStruct((chunks, model, LANES), jnp.float32),
        name="weight",
    )(layer_rows, grad_k)
    low = max(d for d in range(1, count + 1) if count % d == 0 and d * d <= count)
    high, wide = count // low, ranks // 2
    rows = model // (ranks * count)
    half = chunks // 2

    def held(*lead):
        return pltpu.VMEM(lead + (rows, LANES), jnp.float32)

    most = max(wide, high, low)
    vmem = pl.BlockSpec(memory_space=pltpu.VMEM)
    return pl.pallas_call(
        functools.partial(scatter_kernel, (wide, high, low)),
        in_specs=[vmem],
        out_specs=vmem,
        out_shape=jax.ShapeDtypeStruct((rows, columns), jnp.float32),
        scratch_shapes=[
            held(chunks, wide, high, low),
            held(chunks, wide, high, low),
            held(half, wide - 1, high, low),
            held(half, high, low),
            held(half, low - 1, high),
            held(half, low - 1, wide, high),
            held(half, wide, high),
            held(half, wide - 1, high),
            held(chunks, high),
            held(chunks, high - 1),
            pltpu.SemaphoreType.DMA((4, chunks, most - 1)),
            pltpu.SemaphoreType.DMA((4, chunks, most - 1)),
        ],
        compiler_params=pltpu.CompilerParams(collective_id=1, has_side_effects=True),
        name="scatter",
    )(part.reshape(chunks, wide, 2, high, low, rows, LANES))


def shards(counts, queries, key_vectors, value_vectors, grad_output, log_gate, layer_input):
    length = queries.shape[1]
    count = counts[1]
    f32, bf16 = jnp.float32, jnp.bfloat16
    thin = pl.BlockSpec((length, DK), lambda h: (0, h))
    wide = pl.BlockSpec((length, DV), lambda h: (0, h))
    carry = pl.BlockSpec((DV, DK), lambda h: (h, 0))
    rows = (queries[0], key_vectors[0], value_vectors[0], grad_output[0], log_gate[0])
    work = length * DK * DV * HEADS
    decay, forward, backward = pl.pallas_call(
        states_kernel,
        grid=(HEADS,),
        in_specs=[thin, thin, wide, wide, thin],
        out_specs=[pl.BlockSpec((8, DK), lambda h: (h, 0)), carry, carry],
        out_shape=[
            jax.ShapeDtypeStruct((HEADS * 8, DK), f32),
            jax.ShapeDtypeStruct((HEADS * DV, DK), f32),
            jax.ShapeDtypeStruct((HEADS * DV, DK), f32),
        ],
        cost_estimate=pl.CostEstimate(
            flops=4 * work, bytes_accessed=length * HEADS * 24 * DK, transcendentals=0
        ),
        name="states",
    )(*rows)
    chunks = HEADS * DV // ROWS
    vmem = pl.BlockSpec(memory_space=pltpu.VMEM)
    incoming, outgoing = pl.pallas_call(
        functools.partial(chain_kernel, count),
        in_specs=[vmem] * 3,
        out_specs=[vmem] * 2,
        out_shape=[jax.ShapeDtypeStruct((HEADS * DV, DK), f32)] * 2,
        scratch_shapes=[pltpu.VMEM((HEADS * DV, DK), f32)] * 2
        + [pltpu.SemaphoreType.DMA((chunks,))] * 4,
        compiler_params=pltpu.CompilerParams(collective_id=0, has_side_effects=True),
        name="chain",
    )(decay, forward, backward)
    grad_q, grad_k, grad_v, grad_gate = pl.pallas_call(
        grads_kernel,
        grid=(HEADS,),
        in_specs=[thin, thin, wide, wide, thin, carry, carry],
        out_specs=[thin, thin, wide, thin],
        out_shape=[
            jax.ShapeDtypeStruct((length, HEADS * DK), bf16),
            jax.ShapeDtypeStruct((length, HEADS * DK), bf16),
            jax.ShapeDtypeStruct((length, HEADS * DV), bf16),
            jax.ShapeDtypeStruct((length, HEADS * DK), f32),
        ],
        scratch_shapes=[pltpu.VMEM((length, DK), f32)],
        cost_estimate=pl.CostEstimate(
            flops=16 * work, bytes_accessed=length * HEADS * 40 * DK, transcendentals=0
        ),
        name="grads",
    )(*rows, incoming, outgoing)
    grad_key_weight = weight_sum(counts, layer_input[0], grad_k)
    return (grad_q[None], grad_k[None], grad_v[None], grad_gate[None], grad_key_weight)


def solution(mesh):
    rows = P("dp", "seq", None)
    return jax.shard_map(
        functools.partial(shards, (mesh.shape["dp"], mesh.shape["seq"])),
        mesh=mesh,
        in_specs=(rows,) * 6,
        out_specs=(rows, rows, rows, rows, P(("dp", "seq"), None)),
        check_vma=False,
    )
```

```python
import functools

import jax
import jax.numpy as jnp
from jax import lax
from jax.experimental import pallas as pl
from jax.experimental.pallas import tpu as pltpu
from jax.sharding import PartitionSpec as P

HEADS = 4
DK = 256
DV = 512
ROWS = 64
SLACK = 3
LANES = 128
NT = (((1,), (1,)), ((), ()))
TN = (((0,), (0,)), ((), ()))
NN = (((1,), (0,)), ((), ()))


def mm(first_op, second_op, dims):
    return lax.dot_general(
        first_op.astype(jnp.bfloat16),
        second_op.astype(jnp.bfloat16),
        dims,
        preferred_element_type=jnp.float32,
    )


def block_of(length):
    return 128 if length % 128 == 0 else 64


def triangle(size, lower):
    row = lax.broadcasted_iota(jnp.int32, (size, size), 0)
    col = lax.broadcasted_iota(jnp.int32, (size, size), 1)
    return (row >= col) if lower else (row <= col)


def exact_sum(ones, values):
    high = values.astype(jnp.bfloat16)
    rest = values - high.astype(jnp.float32)
    middle = rest.astype(jnp.bfloat16)
    low = (rest - middle.astype(jnp.float32)).astype(jnp.bfloat16)
    return mm(ones, high, NN) + (mm(ones, middle, NN) + mm(ones, low, NN))


def states_kernel(q_ref, k_ref, v_ref, g_ref, lg_ref, decay_ref, f_ref, b_ref):
    length = q_ref.shape[0]
    size = block_of(length)
    ones = triangle(size, True).astype(jnp.bfloat16)
    base = jnp.zeros((1, DK), jnp.float32)
    cums = []
    for n in range(length // size):
        part = exact_sum(ones, lg_ref[n * size : (n + 1) * size, :]) + base
        base = part[size - 1 :, :]
        cums.append(part)
    cum = jnp.concatenate(cums, axis=0)
    decay_ref[...] = jnp.broadcast_to(jnp.exp(base), decay_ref.shape)
    key_end = k_ref[...].astype(jnp.float32) * jnp.exp(base - cum)
    query_up = q_ref[...].astype(jnp.float32) * jnp.exp(cum)
    f_ref[...] = mm(v_ref[...], key_end, TN)
    b_ref[...] = DK**-0.5 * mm(g_ref[...], query_up, TN)


def chain_kernel(
    count, decay_ref, f_ref, b_ref, fin_ref, bin_ref, f_out, b_out, f_send, f_recv, b_send, b_recv
):
    place = lax.axis_index("seq")
    right = lax.rem(place + 1, count)
    left = lax.rem(place + count - 1, count)
    chunks = f_ref.shape[0] // ROWS
    per_head = chunks // HEADS
    barrier = pltpu.get_barrier_semaphore()
    for peer in (left, right):
        pl.semaphore_signal(
            barrier, inc=1, device_id={"seq": peer}, device_id_type=pl.DeviceIdType.MESH
        )
    pl.semaphore_wait(barrier, 2)

    def copy(c, out, into, send, recv, peer):
        rows = pl.ds(pl.multiple_of(c * ROWS, ROWS), ROWS)
        return pltpu.make_async_remote_copy(
            src_ref=out.at[rows],
            dst_ref=into.at[rows],
            send_sem=send.at[c],
            recv_sem=recv.at[c],
            device_id={"seq": peer},
            device_id_type=pl.DeviceIdType.MESH,
        )

    def advance(c, own, out, into, send, recv, peer, is_first, is_last):
        rows = pl.ds(pl.multiple_of(c * ROWS, ROWS), ROWS)

        @pl.when(is_first)
        def _():
            into[rows, :] = jnp.zeros((ROWS, DK), jnp.float32)

        @pl.when(jnp.logical_not(is_first))
        def _():
            copy(c, out, into, send, recv, peer).wait_recv()

        @pl.when(jnp.logical_not(is_last))
        def _():
            decay = decay_ref[pl.ds((c // per_head) * 8, 8), :][0:1, :]
            out[rows, :] = decay * into[rows, :] + own[rows, :]
            copy(c, out, into, send, recv, peer).start()

    at_low, at_high = place == 0, place == count - 1

    def step(t, _):
        ahead = t - SLACK * place
        back = t - SLACK * (count - 1 - place)

        @pl.when((ahead >= 0) & (ahead < chunks))
        def _():
            advance(ahead, f_ref, f_out, fin_ref, f_send, f_recv, right, at_low, at_high)

        @pl.when((back >= 0) & (back < chunks))
        def _():
            advance(back, b_ref, b_out, bin_ref, b_send, b_recv, left, at_high, at_low)

        return 0

    lax.fori_loop(0, chunks + SLACK * (count - 1), step, 0)

    def drain(c, _):
        @pl.when(jnp.logical_not(at_high))
        def _():
            copy(c, f_out, fin_ref, f_send, f_recv, right).wait_send()

        @pl.when(jnp.logical_not(at_low))
        def _():
            copy(c, b_out, bin_ref, b_send, b_recv, left).wait_send()

        return 0

    lax.fori_loop(0, chunks, drain, 0)


def grads_kernel(
    q_ref, k_ref, v_ref, g_ref, lg_ref, fin_ref, bin_ref, dq_ref, dk_ref, dv_ref, gate_ref, dq_full
):
    length = q_ref.shape[0]
    size = block_of(length)
    scale = DK**-0.5
    lower = triangle(size, True)
    sum_down = lower.astype(jnp.bfloat16)
    sum_up = triangle(size, False).astype(jnp.bfloat16)
    state = fin_ref[...]
    back = bin_ref[...]
    kept = []
    for n in range(length // size):
        at = slice(n * size, (n + 1) * size)
        cum = exact_sum(sum_down, lg_ref[at, :])
        end = cum[size - 1 :, :]
        middle = cum[size // 2 - 1 : size // 2, :]
        rise = jnp.exp(cum - middle)
        fall = jnp.exp(middle - cum)
        key = k_ref[at, :].astype(jnp.float32)
        pair = jnp.where(lower, mm(g_ref[at, :], v_ref[at, :], NT), 0.0).astype(jnp.bfloat16)
        dq = scale * (
            jnp.exp(cum) * mm(g_ref[at, :], state, NN) + rise * mm(pair, key * fall, NN)
        )
        dq_full[at, :] = dq
        dq_ref[at, :] = dq.astype(jnp.bfloat16)
        state = state * jnp.exp(end) + mm(v_ref[at, :], key * jnp.exp(end - cum), TN)
        kept.append((cum, pair))
    tail = jnp.sum(state * back, axis=0, keepdims=True)
    for n in reversed(range(length // size)):
        at = slice(n * size, (n + 1) * size)
        cum, pair = kept[n]
        end = cum[size - 1 :, :]
        middle = cum[size // 2 - 1 : size // 2, :]
        rise = jnp.exp(cum - middle)
        fall = jnp.exp(middle - cum)
        to_end = jnp.exp(end - cum)
        query = q_ref[at, :].astype(jnp.float32)
        key = k_ref[at, :].astype(jnp.float32)
        query_rise = (query * rise).astype(jnp.bfloat16)
        scores = jnp.where(lower, scale * mm(query_rise, key * fall, NT), 0.0)
        dk = scale * fall * mm(pair, query_rise, TN) + to_end * mm(v_ref[at, :], back, NN)
        dv = mm(scores, g_ref[at, :], TN) + mm(key * to_end, back, NT)
        dk_ref[at, :] = dk.astype(jnp.bfloat16)
        dv_ref[at, :] = dv.astype(jnp.bfloat16)
        sums = exact_sum(sum_up, query * dq_full[at, :] - key * dk) + tail
        gate_ref[at, :] = sums
        tail = sums[0:1, :]
        back = back * jnp.exp(end) + scale * mm(
            g_ref[at, :], query * jnp.exp(cum), TN
        )


def weight_kernel(x_ref, k_ref, out_ref):
    total = mm(x_ref[...], k_ref[...], TN)
    for c in range(out_ref.shape[0]):
        out_ref[c] = total[:, c * LANES : (c + 1) * LANES]


def scatter_kernel(sizes, part_ref, out_ref, *scratch):
    wide, high, low = sizes
    r0, s0, ry1, sy1, ry2, rb1, sb1, rb2, s2, r3, send, recv = scratch
    chunks = part_ref.shape[0]
    dp, seq = lax.axis_index("dp"), lax.axis_index("seq")
    y, core = dp // 2, dp % 2
    a, b = seq // low, seq % low
    other = 1 - core

    def peers(axis):
        me, size = {"y": (y, wide), "b": (b, low), "a": (a, high)}[axis]
        return [lax.rem(me + k, size) for k in range(1, size)]

    def device(axis, value):
        place = {"y": y, "core": core, "a": a, "b": b} | {axis: value}
        return {"dp": place["y"] * 2 + place["core"], "seq": place["a"] * low + place["b"]}

    barrier = pltpu.get_barrier_semaphore()
    reached = [device("core", other)]
    for axis in ("y", "b", "a"):
        reached += [device(axis, p) for p in peers(axis)]
    for target in reached:
        pl.semaphore_signal(
            barrier, inc=1, device_id=target, device_id_type=pl.DeviceIdType.MESH
        )
    pl.semaphore_wait(barrier, len(reached))

    def copies(c, stage, axis, source, into):
        made = []
        for k, peer in enumerate([other] if axis == "core" else peers(axis)):
            made.append(
                pltpu.make_async_remote_copy(
                    src_ref=source(peer),
                    dst_ref=into(k),
                    send_sem=send.at[stage, c, k],
                    recv_sem=recv.at[stage, c, k],
                    device_id=device(axis, peer),
                    device_id_type=pl.DeviceIdType.MESH,
                )
            )
        return made

    def stage_of(c, stage):
        half = c // 2
        y_first = c % 2 == 0
        if stage == 0:
            return copies(c, 0, "core", lambda p: part_ref.at[c, :, p], lambda k: r0.at[c])
        if stage == 1 and y_first:
            return copies(c, 1, "y", lambda p: s0.at[c, p], lambda k: ry1.at[half, k])
        if stage == 1:
            return copies(c, 1, "b", lambda p: s0.at[c, :, :, p], lambda k: rb1.at[half, k])
        if stage == 2 and y_first:
            return copies(c, 2, "b", lambda p: sy1.at[half, :, p], lambda k: ry2.at[half, k])
        if stage == 2:
            return copies(c, 2, "y", lambda p: sb1.at[half, p], lambda k: rb2.at[half, k])
        return copies(c, 3, "a", lambda p: s2.at[c, p], lambda k: r3.at[c, k])

    def landed(c, stage):
        half = c // 2
        y_first = c % 2 == 0
        for one in stage_of(c, stage):
            one.wait_recv()
        if stage == 0:
            s0[c] = part_ref[c, :, core] + r0[c]
        elif stage == 1 and y_first:
            sy1[half] = sum((ry1[half, k] for k in range(wide - 1)), s0[c, y])
        elif stage == 1:
            sb1[half] = sum((rb1[half, k] for k in range(low - 1)), s0[c, :, :, b])
        elif stage == 2 and y_first:
            s2[c] = sum((ry2[half, k] for k in range(low - 1)), sy1[half, :, b])
        elif stage == 2:
            s2[c] = sum((rb2[half, k] for k in range(wide - 1)), sb1[half, y])
        else:
            out_ref[:, c * LANES : (c + 1) * LANES] = sum(
                (r3[c, k] for k in range(high - 1)), s2[c, a]
            )

    def begin(c, stage):
        for one in stage_of(c, stage):
            one.start()

    for c in range(chunks):
        begin(c, 0)
    for c in range(chunks):
        landed(c, 0)
        begin(c, 1)
    for t in range(chunks + 2):
        for stage in (1, 2, 3):
            c = t - stage + 1
            if 0 <= c < chunks:
                landed(c, stage)
                if stage < 3:
                    begin(c, stage + 1)
    for c in range(chunks):
        for stage in range(4):
            for one in stage_of(c, stage):
                one.wait_send()


def weight_sum(counts, layer_rows, grad_k):
    length, model = layer_rows.shape
    columns = grad_k.shape[1]
    ranks, count = counts
    chunks = columns // LANES
    tall = min(256, model)
    part = pl.pallas_call(
        weight_kernel,
        grid=(model // tall,),
        in_specs=[
            pl.BlockSpec((length, tall), lambda i: (0, i)),
            pl.BlockSpec((length, columns), lambda i: (0, 0)),
        ],
        out_specs=pl.BlockSpec((chunks, tall, LANES), lambda i: (0, i, 0)),
        out_shape=jax.ShapeDtypeStruct((chunks, model, LANES), jnp.float32),
        name="weight",
    )(layer_rows, grad_k)
    low = max(d for d in range(1, count + 1) if count % d == 0 and d * d <= count)
    high, wide = count // low, ranks // 2
    rows = model // (ranks * count)
    half = chunks // 2

    def held(*lead):
        return pltpu.VMEM(lead + (rows, LANES), jnp.float32)

    most = max(wide, high, low)
    vmem = pl.BlockSpec(memory_space=pltpu.VMEM)
    return pl.pallas_call(
        functools.partial(scatter_kernel, (wide, high, low)),
        in_specs=[vmem],
        out_specs=vmem,
        out_shape=jax.ShapeDtypeStruct((rows, columns), jnp.float32),
        scratch_shapes=[
            held(chunks, wide, high, low),
            held(chunks, wide, high, low),
            held(half, wide - 1, high, low),
            held(half, high, low),
            held(half, low - 1, high),
            held(half, low - 1, wide, high),
            held(half, wide, high),
            held(half, wide - 1, high),
            held(chunks, high),
            held(chunks, high - 1),
            pltpu.SemaphoreType.DMA((4, chunks, most - 1)),
            pltpu.SemaphoreType.DMA((4, chunks, most - 1)),
        ],
        compiler_params=pltpu.CompilerParams(collective_id=1, has_side_effects=True),
        name="scatter",
    )(part.reshape(chunks, wide, 2, high, low, rows, LANES))


def shards(counts, queries, key_vectors, value_vectors, grad_output, log_gate, layer_input):
    length = queries.shape[1]
    count = counts[1]
    f32, bf16 = jnp.float32, jnp.bfloat16
    thin = pl.BlockSpec((length, DK), lambda h: (0, h))
    wide = pl.BlockSpec((length, DV), lambda h: (0, h))
    carry = pl.BlockSpec((DV, DK), lambda h: (h, 0))
    rows = (queries[0], key_vectors[0], value_vectors[0], grad_output[0], log_gate[0])
    work = length * DK * DV * HEADS
    decay, forward, backward = pl.pallas_call(
        states_kernel,
        grid=(HEADS,),
        in_specs=[thin, thin, wide, wide, thin],
        out_specs=[pl.BlockSpec((8, DK), lambda h: (h, 0)), carry, carry],
        out_shape=[
            jax.ShapeDtypeStruct((HEADS * 8, DK), f32),
            jax.ShapeDtypeStruct((HEADS * DV, DK), f32),
            jax.ShapeDtypeStruct((HEADS * DV, DK), f32),
        ],
        cost_estimate=pl.CostEstimate(
            flops=4 * work, bytes_accessed=length * HEADS * 24 * DK, transcendentals=0
        ),
        name="states",
    )(*rows)
    chunks = HEADS * DV // ROWS
    vmem = pl.BlockSpec(memory_space=pltpu.VMEM)
    incoming, outgoing = pl.pallas_call(
        functools.partial(chain_kernel, count),
        in_specs=[vmem] * 3,
        out_specs=[vmem] * 2,
        out_shape=[jax.ShapeDtypeStruct((HEADS * DV, DK), f32)] * 2,
        scratch_shapes=[pltpu.VMEM((HEADS * DV, DK), f32)] * 2
        + [pltpu.SemaphoreType.DMA((chunks,))] * 4,
        compiler_params=pltpu.CompilerParams(collective_id=0, has_side_effects=True),
        name="chain",
    )(decay, forward, backward)
    grad_q, grad_k, grad_v, grad_gate = pl.pallas_call(
        grads_kernel,
        grid=(HEADS,),
        in_specs=[thin, thin, wide, wide, thin, carry, carry],
        out_specs=[thin, thin, wide, thin],
        out_shape=[
            jax.ShapeDtypeStruct((length, HEADS * DK), bf16),
            jax.ShapeDtypeStruct((length, HEADS * DK), bf16),
            jax.ShapeDtypeStruct((length, HEADS * DV), bf16),
            jax.ShapeDtypeStruct((length, HEADS * DK), f32),
        ],
        scratch_shapes=[pltpu.VMEM((length, DK), f32)],
        cost_estimate=pl.CostEstimate(
            flops=16 * work, bytes_accessed=length * HEADS * 40 * DK, transcendentals=0
        ),
        name="grads",
    )(*rows, incoming, outgoing)
    grad_key_weight = weight_sum(counts, layer_input[0], grad_k)
    return (grad_q[None], grad_k[None], grad_v[None], grad_gate[None], grad_key_weight)


def solution(mesh):
    rows = P("dp", "seq", None)
    return jax.shard_map(
        functools.partial(shards, (mesh.shape["dp"], mesh.shape["seq"])),
        mesh=mesh,
        in_specs=(rows,) * 6,
        out_specs=(rows, rows, rows, rows, P(("dp", "seq"), None)),
        check_vma=False,
    )
```
